8 devices in a mesh: terms: 8 (over z, y, x, core).
Axes of the slice: x: 2, y: 2, z: 1, core: 2. Of those that a mesh axis runs over, the one named last changes fastest.
Arguments:
- psi: float32 [640, 4, 4, 640], replicated
- left_env: bfloat16 [48, 640, 640], P('terms')
- two_site: bfloat16 [48, 16, 16], P('terms')
- right_env: bfloat16 [48, 640, 640], P('terms')
Outputs:
- output 1: float32 [7, 640, 4, 4, 640], replicated
- output 2: float32 [6], replicated
- output 3: float32 [6], replicated
All inputs are finite; a program needn't handle non-finite values.
Results may differ from the reference program's by a relative error of at most 0.0133512.
Values are sent between devices in bfloat16 or wider.
A program may use at most 1 GiB of HBM per device.

```python
import jax
import jax.numpy as jnp
from jax import lax

BOND_DIM = 640
PHYS_DIM = 4
LANCZOS_STEPS = 6
NUM_TERMS = 48
PAIR_DIM = PHYS_DIM * PHYS_DIM


def sym_draw(key, count, size):
    raw_draw = jax.random.normal(key, (count, size, size), jnp.float32)
    return (raw_draw + jnp.swapaxes(raw_draw, 1, 2)) * (0.5 ** 0.5)


def setup_inputs(seed: int = 0) -> dict:
    keys = jax.random.split(jax.random.key(seed), 4)
    psi = jax.random.normal(keys[0], (BOND_DIM, PHYS_DIM, PHYS_DIM, BOND_DIM), jnp.float32)
    eye_bond = jnp.eye(BOND_DIM, dtype=jnp.float32)
    left_env = eye_bond + sym_draw(keys[1], NUM_TERMS, BOND_DIM) * BOND_DIM ** -0.5
    two_site = sym_draw(keys[2], NUM_TERMS, PAIR_DIM) * (PAIR_DIM * NUM_TERMS) ** -0.5
    right_env = eye_bond + sym_draw(keys[3], NUM_TERMS, BOND_DIM) * BOND_DIM ** -0.5
    return {"psi": psi, "left_env": left_env.astype(jnp.bfloat16), "two_site": two_site.astype(jnp.bfloat16), "right_env": right_env.astype(jnp.bfloat16)}


def apply_ham(vec_bf, left_env, two_site, right_env):
    vec_flat = vec_bf.reshape(BOND_DIM * PAIR_DIM, BOND_DIM)

    def one_term(acc_sum, term):
        left_k, site_k, right_k = term
        right_out = jnp.dot(vec_flat, right_k.T, preferred_element_type=jnp.float32).astype(jnp.bfloat16)
        site_out = jnp.einsum("qp,xpb->xqb", site_k.astype(jnp.float32), right_out.reshape(BOND_DIM, PAIR_DIM, BOND_DIM).astype(jnp.float32)).astype(jnp.bfloat16)
        left_out = jnp.dot(left_k, site_out.reshape(BOND_DIM, PAIR_DIM * BOND_DIM), preferred_element_type=jnp.float32)
        return acc_sum + left_out, None

    init_acc = jnp.zeros((BOND_DIM, PAIR_DIM * BOND_DIM), jnp.float32)
    total = lax.scan(one_term, init_acc, (left_env, two_site, right_env))[0]
    return total.reshape(BOND_DIM, PHYS_DIM, PHYS_DIM, BOND_DIM)


def reference(psi, left_env, two_site, right_env):
    cur_vec = psi / jnp.sqrt(jnp.sum(psi * psi))
    prev_vec = jnp.zeros_like(cur_vec)
    beta_prev = 0.0
    vectors = [cur_vec]
    alphas = []
    betas = []
    for step_idx in range(LANCZOS_STEPS):
        sigma = apply_ham(cur_vec.astype(jnp.bfloat16), left_env, two_site, right_env)
        alpha = jnp.sum(sigma * cur_vec)
        residual = sigma - alpha * cur_vec - beta_prev * prev_vec
        beta = jnp.sqrt(jnp.sum(residual * residual))
        prev_vec = cur_vec
        cur_vec = residual / beta
        vectors.append(cur_vec)
        alphas.append(alpha)
        betas.append(beta)
        beta_prev = beta
    return (jnp.stack(vectors), jnp.stack(alphas), jnp.stack(betas))
```

```python
import functools

import jax
import jax.numpy as jnp
from jax import lax
from jax.experimental import pallas as pl
from jax.experimental.pallas import tpu as pltpu
from jax.sharding import PartitionSpec as P

LANCZOS_STEPS = 6
LANE = 128
SUB = 16
GROUP = 6
PIECES = (2, 3)
MESH = pl.DeviceIdType.MESH


def ham_kernel(bond, pair, slab, group, first, u_ref, r_ref, w_ref, l_ref, *rest):
    out_ref, y1, y2 = rest[-3:]
    inner = u_ref.shape[1] // (pair * LANE)
    chunks = bond // LANE
    bgroups = slab // SUB
    width = pair * LANE

    @pl.when(pl.program_id(0) == 0)
    def _():
        out_ref[...] = jnp.zeros_like(out_ref) if first else rest[0][...]

    def right(i, _):
        cols = pl.ds(pl.multiple_of(i * width, width), width)
        y1[:, cols] = jnp.dot(r_ref[...], u_ref[:, cols], preferred_element_type=jnp.float32).astype(jnp.bfloat16)
        return 0

    lax.fori_loop(0, inner, right, 0, unroll=True)

    blocks = [(bg, ac) for bg in range(bgroups) for ac in range(inner)]

    def site(k, _):
        w_k = w_ref[k]
        base = k * slab
        for start in range(0, len(blocks), 4):
            part = blocks[start : start + 4]
            tiles = []
            for bg, ac in part:
                sub = pl.ds(pl.multiple_of(base + bg * SUB, SUB), SUB)
                tiles.append(jnp.concatenate([y1[sub, (ac * pair + p) * LANE : (ac * pair + p + 1) * LANE] for p in range(pair)], axis=0))
            rhs = tiles[0] if len(tiles) == 1 else jnp.concatenate(tiles, axis=1)
            res = jnp.dot(w_k, rhs, preferred_element_type=jnp.float32).astype(jnp.bfloat16)
            for n, (bg, ac) in enumerate(part):
                cols = pl.ds(pl.multiple_of((k * inner + ac) * LANE, LANE), LANE)
                for q in range(pair):
                    y2[q * slab + bg * SUB : q * slab + (bg + 1) * SUB, cols] = res[q * SUB : (q + 1) * SUB, n * LANE : (n + 1) * LANE]
        return 0

    lax.fori_loop(0, group, site, 0, unroll=True)

    qs = pair // 2

    def left(i, _):
        sub = pl.ds(pl.multiple_of(i * (qs * slab), qs * slab), qs * slab)
        res = jnp.dot(y2[sub, :], l_ref[...], preferred_element_type=jnp.float32)
        for ac in range(chunks):
            for n in range(qs):
                cols = pl.ds(pl.multiple_of((ac * pair + n) * LANE + i * (qs * LANE), LANE), LANE)
                out_ref[:, cols] += res[n * slab : (n + 1) * slab, ac * LANE : (ac + 1) * LANE]
        return 0

    lax.fori_loop(0, pair // qs, left, 0, unroll=True)


def apply_ham(u_part, right_rows, site_kron, left_rows, sigma, pair, slab):
    bond = u_part.shape[0]
    terms = site_kron.shape[0]
    side = pair * SUB
    span = u_part.shape[1] // pair
    full = lambda i: (0, 0)
    flops = 2 * terms * slab * (bond * span * pair * 2 + side * side * span // SUB)
    once = pl.BlockSpec((slab, bond * pair), full, pipeline_mode=pl.Buffered(1))
    first = sigma is None
    return pl.pallas_call(
        functools.partial(ham_kernel, bond, pair, slab, GROUP, first),
        grid=(terms // GROUP,),
        in_specs=[
            pl.BlockSpec((bond, span * pair), full, pipeline_mode=pl.Buffered(1)),
            pl.BlockSpec((GROUP * slab, bond), lambda i: (i, 0)),
            pl.BlockSpec((GROUP, side, side), lambda i: (i, 0, 0)),
            pl.BlockSpec((GROUP * span, bond), lambda i: (i, 0)),
        ] + ([] if first else [once]),
        out_specs=once,
        out_shape=jax.ShapeDtypeStruct((slab, bond * pair), jnp.float32),
        scratch_shapes=[
            pltpu.VMEM((GROUP * slab, span * pair), jnp.bfloat16),
            pltpu.VMEM((pair * slab, GROUP * span), jnp.bfloat16),
        ],
        compiler_params=pltpu.CompilerParams(dimension_semantics=("arbitrary",), vmem_limit_bytes=60_000_000),
        cost_estimate=pl.CostEstimate(flops=flops, bytes_accessed=50_000_000, transcendentals=0),
        name="apply_ham",
    )(u_part, right_rows, site_kron, left_rows, *([] if first else [sigma]))


def update_kernel(devices, sig_ref, cur_ref, prev_ref, bprev_ref, nxt_ref, alpha_ref, beta_ref, *rest):
    low_refs, (parts, slots, send_sem, recv_sem) = rest[:-4], rest[-4:]
    me = lax.axis_index("terms")
    rows, cols = sig_ref.shape
    step = 512

    barrier = pltpu.get_barrier_semaphore()
    for off in range(1, devices):
        pl.semaphore_signal(barrier, inc=1, device_id=(lax.rem(me + off, devices),), device_id_type=MESH)

    def fold(val):
        return val.reshape(rows // 8, 8, step // LANE, LANE).sum(axis=(0, 2))

    def view(i):
        return pl.ds(pl.multiple_of(i * step, step), step)

    def all_sum(phase):
        slots[phase, me] = parts[phase]
        copies = []
        for off in range(1, devices):
            copies.append(pltpu.make_async_remote_copy(
                src_ref=parts.at[phase],
                dst_ref=slots.at[phase, me],
                send_sem=send_sem.at[phase, off],
                recv_sem=recv_sem.at[phase, off],
                device_id=(lax.rem(me + off, devices),),
                device_id_type=MESH,
            ))
        for copy in copies:
            copy.start()
        for copy in copies:
            copy.wait()
        total = slots[phase, 0]
        for dev in range(1, devices):
            total = total + slots[phase, dev]
        return jnp.sum(jnp.sum(total, axis=0, keepdims=True), axis=1, keepdims=True)

    zero = jnp.zeros((8, LANE), jnp.float32)

    def dot_part(i, acc):
        return acc + fold(sig_ref[:, view(i)] * cur_ref[:, view(i)])

    parts[0] = lax.fori_loop(0, cols // step, dot_part, zero)
    pl.semaphore_wait(barrier, devices - 1)
    alpha = all_sum(0)
    beta_prev = bprev_ref[0:1, 0:1]

    def residual(i, acc):
        res = sig_ref[:, view(i)] - alpha * cur_ref[:, view(i)] - beta_prev * prev_ref[:, view(i)]
        nxt_ref[:, view(i)] = res
        return acc + fold(res * res)

    parts[1] = lax.fori_loop(0, cols // step, residual, zero)
    beta = jnp.sqrt(all_sum(1))

    def scale(i, _):
        val = nxt_ref[:, view(i)] / beta
        nxt_ref[:, view(i)] = val
        return val.astype(jnp.bfloat16)

    base = 0
    for low_ref in low_refs:
        def piece(i, _, base=base, low_ref=low_ref):
            low_ref[:, view(i)] = scale(i + base, 0)
            return 0

        count = low_ref.shape[1] // step
        lax.fori_loop(0, count, piece, 0)
        base += count
    if not low_refs:
        def only(i, _):
            scale(i, 0)
            return 0

        lax.fori_loop(0, cols // step, only, 0)
    alpha_ref[...] = jnp.broadcast_to(alpha, alpha_ref.shape)
    beta_ref[...] = jnp.broadcast_to(beta, beta_ref.shape)


def update(devices, widths, sigma, cur, prev, beta_prev):
    vmem = pl.BlockSpec(memory_space=pltpu.VMEM)
    shape = sigma.shape
    return pl.pallas_call(
        functools.partial(update_kernel, devices),
        out_shape=[
            jax.ShapeDtypeStruct(shape, jnp.float32),
            jax.ShapeDtypeStruct((8, LANE), jnp.float32),
            jax.ShapeDtypeStruct((8, LANE), jnp.float32),
        ] + [jax.ShapeDtypeStruct((shape[0], width), jnp.bfloat16) for width in widths],
        in_specs=[vmem] * 4,
        out_specs=[vmem] * (3 + len(widths)),
        scratch_shapes=[
            pltpu.VMEM((2, 8, LANE), jnp.float32),
            pltpu.VMEM((2, devices, 8, LANE), jnp.float32),
            pltpu.SemaphoreType.DMA((2, devices)),
            pltpu.SemaphoreType.DMA((2, devices)),
        ],
        compiler_params=pltpu.CompilerParams(collective_id=0 if widths else 1, has_side_effects=True, vmem_limit_bytes=32_000_000),
        cost_estimate=pl.CostEstimate(flops=20_000_000, bytes_accessed=20_000_000, transcendentals=0),
        name="lanczos_update",
    )(sigma, cur, prev, beta_prev)


def out_kernel(phys, rows_ref, kry_ref, out_ref, tmp):
    pair = phys * phys
    bond = rows_ref.shape[0]
    planes = bond // LANE
    for q in range(pair):
        for j in range(planes):
            tmp[j, pl.ds(q, LANE, stride=pair), :] = rows_ref[j * LANE : (j + 1) * LANE, q * LANE : (q + 1) * LANE].T

    def put(a, _):
        for n in range(4):
            row = a * 4 + n
            for j in range(planes):
                val = tmp[j, pl.ds(pl.multiple_of(row * pair, pair), pair), :]
                for s in range(phys):
                    out_ref[0, row, s, :, j * LANE : (j + 1) * LANE] = val[s * phys : (s + 1) * phys, :]
        return 0

    lax.fori_loop(0, LANE // 4, put, 0)

def write_vector(kry, rows, index, first=0):
    phys, bond = kry.shape[2], kry.shape[4]
    pair = phys * phys
    return pl.pallas_call(
        functools.partial(out_kernel, phys),
        grid=(rows.shape[1] // (pair * LANE),),
        in_specs=[pl.BlockSpec((bond, pair * LANE), lambda i: (0, i)), pl.BlockSpec(memory_space=pl.ANY)],
        out_specs=pl.BlockSpec((1, LANE, phys, phys, bond), lambda i: (index, i + first, 0, 0, 0)),
        out_shape=jax.ShapeDtypeStruct(kry.shape, kry.dtype),
        scratch_shapes=[pltpu.VMEM((bond // LANE, LANE * pair, LANE), jnp.float32)],
        input_output_aliases={1: 0},
        compiler_params=pltpu.CompilerParams(dimension_semantics=("arbitrary",), vmem_limit_bytes=48_000_000),
        cost_estimate=pl.CostEstimate(flops=30_000_000, bytes_accessed=54_000_000, transcendentals=0),
        name="write_vector",
    )(rows, kry)


def start_kernel(phys, slab, psi_ref, norm_ref, kry_ref, low_ref, cur_ref, tmp, turned):
    pair = phys * phys
    bond = psi_ref.shape[-1]
    planes = bond // LANE
    me = lax.axis_index("terms")
    norm = norm_ref[0:1, 0:1]

    def put(a, _):
        for n in range(4):
            row = a * 4 + n
            for s in range(phys):
                val = psi_ref[row, s] / norm
                kry_ref[0, row, s] = val
                for j in range(planes):
                    tmp[j, pl.ds(row * pair + s * phys, phys), :] = val[:, j * LANE : (j + 1) * LANE]
        return 0

    lax.fori_loop(0, LANE // 4, put, 0)
    for q in range(pair):
        for j in range(planes):
            val = tmp[j, pl.ds(q, LANE, stride=pair), :].T
            turned[j * LANE : (j + 1) * LANE, q * LANE : (q + 1) * LANE] = val
            low_ref[j * LANE : (j + 1) * LANE, q * LANE : (q + 1) * LANE] = val.astype(jnp.bfloat16)
    cur_ref[...] = turned[pl.ds(pl.multiple_of(me * slab, 8), slab), :]


def start_vectors(psi, norm, count, slab):
    phys, bond = psi.shape[1], psi.shape[3]
    pair = phys * phys
    return pl.pallas_call(
        functools.partial(start_kernel, phys, slab),
        grid=(bond // LANE,),
        in_specs=[pl.BlockSpec((LANE, phys, phys, bond), lambda i: (i, 0, 0, 0)), pl.BlockSpec((1, LANE), lambda i: (0, 0))],
        out_specs=[
            pl.BlockSpec((1, LANE, phys, phys, bond), lambda i: (0, i, 0, 0, 0)),
            pl.BlockSpec((bond, pair * LANE), lambda i: (0, i)),
            pl.BlockSpec((slab, pair * LANE), lambda i: (0, i)),
        ],
        out_shape=[
            jax.ShapeDtypeStruct((count,) + psi.shape, jnp.float32),
            jax.ShapeDtypeStruct((bond, bond * pair), jnp.bfloat16),
            jax.ShapeDtypeStruct((slab, bond * pair), jnp.float32),
        ],
        scratch_shapes=[pltpu.VMEM((bond // LANE, LANE * pair, LANE), jnp.float32), pltpu.VMEM((bond, pair * LANE), jnp.float32)],
        compiler_params=pltpu.CompilerParams(dimension_semantics=("arbitrary",), vmem_limit_bytes=56_000_000),
        cost_estimate=pl.CostEstimate(flops=60_000_000, bytes_accessed=70_000_000, transcendentals=0),
        name="start_vectors",
    )(psi, norm)


def solution(mesh):
    groups = mesh.shape["terms"]

    def body(psi, left_loc, site_loc, right_loc):
        bond, phys = psi.shape[0], psi.shape[1]
        pair = phys * phys
        slab = bond // groups
        chunks = bond // LANE
        row_start = lax.axis_index("terms") * slab

        bounds = [sum(PIECES[:n]) * LANE for n in range(len(PIECES) + 1)]
        spans = list(zip(bounds[:-1], bounds[1:]))
        widths = [(hi - lo) * pair for lo, hi in spans]
        site_all = lax.all_gather(site_loc, "terms", axis=0, tiled=True)
        left_loc, site_all = lax.optimization_barrier((left_loc, site_all))
        lefts = [lax.all_gather(left_loc[:, lo:hi], "terms", axis=0, tiled=True).reshape(-1, bond) for lo, hi in spans]
        right_rows = lax.all_to_all(right_loc, "terms", 1, 0, tiled=True).reshape(-1, bond)
        eye = jnp.eye(SUB, dtype=jnp.bfloat16)
        site_kron = (site_all[:, :, None, :, None] * eye[None, None, :, None, :]).reshape(-1, pair * SUB, pair * SUB)

        norm = jnp.broadcast_to(jnp.sqrt(jnp.sum(psi * psi)), (1, LANE))
        krylov, u_full, cur = start_vectors(psi, norm, LANCZOS_STEPS + 1, slab)
        prev = jnp.zeros_like(cur)
        beta = jnp.zeros((8, LANE), jnp.float32)
        us = [u_full[:, lo * pair : hi * pair] for lo, hi in spans]
        full = None
        alphas = []
        betas = []
        for step_idx in range(LANCZOS_STEPS):
            last = step_idx == LANCZOS_STEPS - 1
            sigma = None
            for u_part, left_rows in zip(us, lefts):
                sigma = apply_ham(u_part, right_rows, site_kron, left_rows, sigma, pair, slab)
            nxt, alpha, beta, *lows = update(groups, () if last else widths, sigma, cur, prev, beta)
            late = nxt
            if full is not None:
                if last:
                    late, full = lax.optimization_barrier((late, full))
                else:
                    lows[0], full = lax.optimization_barrier((lows[0], full))
            if not last:
                us = [lax.all_gather(lows[0], "terms", axis=0, tiled=True)]
            if full is not None:
                krylov = write_vector(krylov, full, step_idx)
                if not last:
                    krylov, lows[1] = lax.optimization_barrier((krylov, lows[1]))
            if not last:
                *lows, late, us[0] = lax.optimization_barrier((*lows[1:], nxt, us[0]))
                us += [lax.all_gather(low, "terms", axis=0, tiled=True) for low in lows]
                full = lax.all_gather(late, "terms", axis=0, tiled=True)
            prev, cur = cur, nxt
            alphas.append(alpha[0, 0])
            betas.append(beta[0, 0])
        cut = 3 * pair * LANE
        head = lax.all_gather(late[:, :cut], "terms", axis=0, tiled=True)
        tail = lax.all_gather(late[:, cut:], "terms", axis=0, tiled=True)
        krylov = write_vector(krylov, head, LANCZOS_STEPS)
        krylov = write_vector(krylov, tail, LANCZOS_STEPS, cut // (pair * LANE))
        return krylov, jnp.stack(alphas), jnp.stack(betas)

    return jax.shard_map(body, mesh=mesh, in_specs=(P(), P("terms"), P("terms"), P("terms")), out_specs=(P(), P(), P()), check_vma=False)
```

```python
import functools

import jax
import jax.numpy as jnp
from jax import lax
from jax.experimental import pallas as pl
from jax.experimental.pallas import tpu as pltpu
from jax.sharding import PartitionSpec as P

LANCZOS_STEPS = 6
LANE = 128
SUB = 16
GROUP = 6
PIECES = ((2,), (2, 1))
MESH = pl.DeviceIdType.MESH


def ham_kernel(bond, pair, slab, group, first, u_ref, r_ref, w_ref, *rest):
    out_ref, y1, y2 = rest[-3:]
    l_refs = rest[:-3] if first else rest[:-4]
    inner = u_ref.shape[1] // (pair * LANE)
    chunks = bond // LANE
    bgroups = slab // SUB
    width = pair * LANE

    @pl.when(pl.program_id(0) == 0)
    def _():
        out_ref[...] = jnp.zeros_like(out_ref) if first else rest[-4][...]

    def right(i, _):
        cols = pl.ds(pl.multiple_of(i * width, width), width)
        y1[:, cols] = jnp.dot(r_ref[...], u_ref[:, cols], preferred_element_type=jnp.float32).astype(jnp.bfloat16)
        return 0

    lax.fori_loop(0, inner, right, 0, unroll=True)

    parts = []
    for l_ref in l_refs:
        size = l_ref.shape[0] // (group * LANE)
        parts.append((sum(n for _, n in parts), size))
    place = {lo + n: (lo * group + n, size) for lo, size in parts for n in range(size)}
    blocks = [(bg, ac) for bg in range(bgroups) for ac in range(inner)]

    def site(k, _):
        w_k = w_ref[k]
        base = k * slab
        for start in range(0, len(blocks), 4):
            part = blocks[start : start + 4]
            tiles = []
            for bg, ac in part:
                sub = pl.ds(pl.multiple_of(base + bg * SUB, SUB), SUB)
                tiles.append(jnp.concatenate([y1[sub, (ac * pair + p) * LANE : (ac * pair + p + 1) * LANE] for p in range(pair)], axis=0))
            rhs = tiles[0] if len(tiles) == 1 else jnp.concatenate(tiles, axis=1)
            res = jnp.dot(w_k, rhs, preferred_element_type=jnp.float32).astype(jnp.bfloat16)
            for n, (bg, ac) in enumerate(part):
                lead, size = place[ac]
                cols = pl.ds(pl.multiple_of((lead + k * size) * LANE, LANE), LANE)
                for q in range(pair):
                    y2[q * slab + bg * SUB : q * slab + (bg + 1) * SUB, cols] = res[q * SUB : (q + 1) * SUB, n * LANE : (n + 1) * LANE]
        return 0

    lax.fori_loop(0, group, site, 0, unroll=True)

    qs = pair // 2

    def left(i, _):
        sub = pl.ds(pl.multiple_of(i * (qs * slab), qs * slab), qs * slab)
        res = 0.0
        for l_ref, (lo, size) in zip(l_refs, parts):
            res += jnp.dot(y2[sub, lo * group * LANE : (lo + size) * group * LANE], l_ref[...], preferred_element_type=jnp.float32)
        for ac in range(chunks):
            for n in range(qs):
                cols = pl.ds(pl.multiple_of((ac * pair + n) * LANE + i * (qs * LANE), LANE), LANE)
                out_ref[:, cols] += res[n * slab : (n + 1) * slab, ac * LANE : (ac + 1) * LANE]
        return 0

    lax.fori_loop(0, pair // qs, left, 0, unroll=True)


def apply_ham(u_part, right_rows, site_kron, left_rows, sigma, pair, slab):
    bond = u_part.shape[0]
    terms = site_kron.shape[0]
    side = pair * SUB
    span = u_part.shape[1] // pair
    full = lambda i: (0, 0)
    flops = 2 * terms * slab * (bond * span * pair * 2 + side * side * span // SUB)
    once = pl.BlockSpec((slab, bond * pair), full, pipeline_mode=pl.Buffered(1))
    first = sigma is None
    return pl.pallas_call(
        functools.partial(ham_kernel, bond, pair, slab, GROUP, first),
        grid=(terms // GROUP,),
        in_specs=[
            pl.BlockSpec((bond, span * pair), full, pipeline_mode=pl.Buffered(1)),
            pl.BlockSpec((GROUP * slab, bond), lambda i: (i, 0)),
            pl.BlockSpec((GROUP, side, side), lambda i: (i, 0, 0)),
        ] + [pl.BlockSpec((GROUP * rows.shape[0] // terms, bond), lambda i: (i, 0)) for rows in left_rows] + ([] if first else [once]),
        out_specs=once,
        out_shape=jax.ShapeDtypeStruct((slab, bond * pair), jnp.float32),
        scratch_shapes=[
            pltpu.VMEM((GROUP * slab, span * pair), jnp.bfloat16),
            pltpu.VMEM((pair * slab, GROUP * span), jnp.bfloat16),
        ],
        compiler_params=pltpu.CompilerParams(dimension_semantics=("arbitrary",), vmem_limit_bytes=60_000_000),
        cost_estimate=pl.CostEstimate(flops=flops, bytes_accessed=50_000_000, transcendentals=0),
        name="apply_ham",
    )(u_part, right_rows, site_kron, *left_rows, *([] if first else [sigma]))


def update_kernel(devices, sig_ref, cur_ref, prev_ref, bprev_ref, nxt_ref, alpha_ref, beta_ref, *rest):
    low_refs, (parts, slots, send_sem, recv_sem) = rest[:-4], rest[-4:]
    me = lax.axis_index("terms")
    rows, cols = sig_ref.shape
    step = 512

    barrier = pltpu.get_barrier_semaphore()
    for off in range(1, devices):
        pl.semaphore_signal(barrier, inc=1, device_id=(lax.rem(me + off, devices),), device_id_type=MESH)

    def fold(val):
        return val.reshape(rows // 8, 8, step // LANE, LANE).sum(axis=(0, 2))

    def view(i):
        return pl.ds(pl.multiple_of(i * step, step), step)

    def all_sum(phase):
        slots[phase, me] = parts[phase]
        copies = []
        for off in range(1, devices):
            copies.append(pltpu.make_async_remote_copy(
                src_ref=parts.at[phase],
                dst_ref=slots.at[phase, me],
                send_sem=send_sem.at[phase, off],
                recv_sem=recv_sem.at[phase, off],
                device_id=(lax.rem(me + off, devices),),
                device_id_type=MESH,
            ))
        for copy in copies:
            copy.start()
        for copy in copies:
            copy.wait()
        total = slots[phase, 0]
        for dev in range(1, devices):
            total = total + slots[phase, dev]
        return jnp.sum(jnp.sum(total, axis=0, keepdims=True), axis=1, keepdims=True)

    zero = jnp.zeros((8, LANE), jnp.float32)

    def dot_part(i, acc):
        return acc + fold(sig_ref[:, view(i)] * cur_ref[:, view(i)])

    parts[0] = lax.fori_loop(0, cols // step, dot_part, zero)
    pl.semaphore_wait(barrier, devices - 1)
    alpha = all_sum(0)
    beta_prev = bprev_ref[0:1, 0:1]

    def residual(i, acc):
        res = sig_ref[:, view(i)] - alpha * cur_ref[:, view(i)] - beta_prev * prev_ref[:, view(i)]
        nxt_ref[:, view(i)] = res
        return acc + fold(res * res)

    parts[1] = lax.fori_loop(0, cols // step, residual, zero)
    beta = jnp.sqrt(all_sum(1))

    def scale(i, _):
        val = nxt_ref[:, view(i)] / beta
        nxt_ref[:, view(i)] = val
        return val.astype(jnp.bfloat16)

    base = 0
    for low_ref in low_refs:
        def piece(i, _, base=base, low_ref=low_ref):
            low_ref[:, view(i)] = scale(i + base, 0)
            return 0

        count = low_ref.shape[1] // step
        lax.fori_loop(0, count, piece, 0)
        base += count
    if not low_refs:
        def only(i, _):
            scale(i, 0)
            return 0

        lax.fori_loop(0, cols // step, only, 0)
    alpha_ref[...] = jnp.broadcast_to(alpha, alpha_ref.shape)
    beta_ref[...] = jnp.broadcast_to(beta, beta_ref.shape)


def update(devices, widths, sigma, cur, prev, beta_prev):
    vmem = pl.BlockSpec(memory_space=pltpu.VMEM)
    shape = sigma.shape
    return pl.pallas_call(
        functools.partial(update_kernel, devices),
        out_shape=[
            jax.ShapeDtypeStruct(shape, jnp.float32),
            jax.ShapeDtypeStruct((8, LANE), jnp.float32),
            jax.ShapeDtypeStruct((8, LANE), jnp.float32),
        ] + [jax.ShapeDtypeStruct((shape[0], width), jnp.bfloat16) for width in widths],
        in_specs=[vmem] * 4,
        out_specs=[vmem] * (3 + len(widths)),
        scratch_shapes=[
            pltpu.VMEM((2, 8, LANE), jnp.float32),
            pltpu.VMEM((2, devices, 8, LANE), jnp.float32),
            pltpu.SemaphoreType.DMA((2, devices)),
            pltpu.SemaphoreType.DMA((2, devices)),
        ],
        compiler_params=pltpu.CompilerParams(collective_id=0 if widths else 1, has_side_effects=True, vmem_limit_bytes=32_000_000),
        cost_estimate=pl.CostEstimate(flops=20_000_000, bytes_accessed=20_000_000, transcendentals=0),
        name="lanczos_update",
    )(sigma, cur, prev, beta_prev)


def out_kernel(phys, rows_ref, kry_ref, out_ref, tmp):
    pair = phys * phys
    bond = rows_ref.shape[0]
    planes = bond // LANE
    for q in range(pair):
        for j in range(planes):
            tmp[j, pl.ds(q, LANE, stride=pair), :] = rows_ref[j * LANE : (j + 1) * LANE, q * LANE : (q + 1) * LANE].T

    def put(a, _):
        for n in range(4):
            row = a * 4 + n
            for j in range(planes):
                val = tmp[j, pl.ds(pl.multiple_of(row * pair, pair), pair), :]
                for s in range(phys):
                    out_ref[0, row, s, :, j * LANE : (j + 1) * LANE] = val[s * phys : (s + 1) * phys, :]
        return 0

    lax.fori_loop(0, LANE // 4, put, 0)

def write_vector(kry, rows, index, first=0):
    phys, bond = kry.shape[2], kry.shape[4]
    pair = phys * phys
    return pl.pallas_call(
        functools.partial(out_kernel, phys),
        grid=(rows.shape[1] // (pair * LANE),),
        in_specs=[pl.BlockSpec((bond, pair * LANE), lambda i: (0, i)), pl.BlockSpec(memory_space=pl.ANY)],
        out_specs=pl.BlockSpec((1, LANE, phys, phys, bond), lambda i: (index, i + first, 0, 0, 0)),
        out_shape=jax.ShapeDtypeStruct(kry.shape, kry.dtype),
        scratch_shapes=[pltpu.VMEM((bond // LANE, LANE * pair, LANE), jnp.float32)],
        input_output_aliases={1: 0},
        compiler_params=pltpu.CompilerParams(dimension_semantics=("arbitrary",), vmem_limit_bytes=48_000_000),
        cost_estimate=pl.CostEstimate(flops=30_000_000, bytes_accessed=54_000_000, transcendentals=0),
        name="write_vector",
    )(rows, kry)


def start_kernel(phys, slab, psi_ref, norm_ref, kry_ref, low_ref, cur_ref, tmp, turned):
    pair = phys * phys
    bond = psi_ref.shape[-1]
    planes = bond // LANE
    me = lax.axis_index("terms")
    norm = norm_ref[0:1, 0:1]

    def put(a, _):
        for n in range(4):
            row = a * 4 + n
            for s in range(phys):
                val = psi_ref[row, s] / norm
                kry_ref[0, row, s] = val
                for j in range(planes):
                    tmp[j, pl.ds(row * pair + s * phys, phys), :] = val[:, j * LANE : (j + 1) * LANE]
        return 0

    lax.fori_loop(0, LANE // 4, put, 0)
    for q in range(pair):
        for j in range(planes):
            val = tmp[j, pl.ds(q, LANE, stride=pair), :].T
            turned[j * LANE : (j + 1) * LANE, q * LANE : (q + 1) * LANE] = val
            low_ref[j * LANE : (j + 1) * LANE, q * LANE : (q + 1) * LANE] = val.astype(jnp.bfloat16)
    cur_ref[...] = turned[pl.ds(pl.multiple_of(me * slab, 8), slab), :]


def start_vectors(psi, norm, count, slab):
    phys, bond = psi.shape[1], psi.shape[3]
    pair = phys * phys
    return pl.pallas_call(
        functools.partial(start_kernel, phys, slab),
        grid=(bond // LANE,),
        in_specs=[pl.BlockSpec((LANE, phys, phys, bond), lambda i: (i, 0, 0, 0)), pl.BlockSpec((1, LANE), lambda i: (0, 0))],
        out_specs=[
            pl.BlockSpec((1, LANE, phys, phys, bond), lambda i: (0, i, 0, 0, 0)),
            pl.BlockSpec((bond, pair * LANE), lambda i: (0, i)),
            pl.BlockSpec((slab, pair * LANE), lambda i: (0, i)),
        ],
        out_shape=[
            jax.ShapeDtypeStruct((count,) + psi.shape, jnp.float32),
            jax.ShapeDtypeStruct((bond, bond * pair), jnp.bfloat16),
            jax.ShapeDtypeStruct((slab, bond * pair), jnp.float32),
        ],
        scratch_shapes=[pltpu.VMEM((bond // LANE, LANE * pair, LANE), jnp.float32), pltpu.VMEM((bond, pair * LANE), jnp.float32)],
        compiler_params=pltpu.CompilerParams(dimension_semantics=("arbitrary",), vmem_limit_bytes=56_000_000),
        cost_estimate=pl.CostEstimate(flops=60_000_000, bytes_accessed=70_000_000, transcendentals=0),
        name="start_vectors",
    )(psi, norm)


def solution(mesh):
    groups = mesh.shape["terms"]

    def body(psi, left_loc, site_loc, right_loc):
        bond, phys = psi.shape[0], psi.shape[1]
        pair = phys * phys
        slab = bond // groups
        chunks = bond // LANE
        row_start = lax.axis_index("terms") * slab

        def ranges(sizes):
            ends = [sum(sizes[: n + 1]) * LANE for n in range(len(sizes))]
            return list(zip([0] + ends[:-1], ends))

        fine = ranges([n for piece in PIECES for n in piece])
        spans = ranges([sum(piece) for piece in PIECES])
        widths = [(hi - lo) * pair for lo, hi in spans]
        site_all = lax.all_gather(site_loc, "terms", axis=0, tiled=True)
        left_loc, site_all = lax.optimization_barrier((left_loc, site_all))
        singles = [[lax.all_gather(left_loc[:, lo:hi], "terms", axis=0, tiled=True).reshape(-1, bond)] for lo, hi in fine]
        lefts = [[rows[0] for rows, (start, _) in zip(singles, fine) if lo <= start < hi] for lo, hi in spans]
        right_rows = lax.all_to_all(right_loc, "terms", 1, 0, tiled=True).reshape(-1, bond)
        eye = jnp.eye(SUB, dtype=jnp.bfloat16)
        site_kron = (site_all[:, :, None, :, None] * eye[None, None, :, None, :]).reshape(-1, pair * SUB, pair * SUB)

        norm = jnp.broadcast_to(jnp.sqrt(jnp.sum(psi * psi)), (1, LANE))
        krylov, u_full, cur = start_vectors(psi, norm, LANCZOS_STEPS + 1, slab)
        prev = jnp.zeros_like(cur)
        beta = jnp.zeros((8, LANE), jnp.float32)
        us = [u_full[:, lo * pair : hi * pair] for lo, hi in fine]
        full = None
        alphas = []
        betas = []
        for step_idx in range(LANCZOS_STEPS):
            last = step_idx == LANCZOS_STEPS - 1
            sigma = None
            for u_part, left_rows in zip(us, lefts if step_idx else singles):
                sigma = apply_ham(u_part, right_rows, site_kron, left_rows, sigma, pair, slab)
            nxt, alpha, beta, *lows = update(groups, () if last else widths, sigma, cur, prev, beta)
            late = nxt
            if full is not None:
                if last:
                    late, full = lax.optimization_barrier((late, full))
                else:
                    lows[0], full = lax.optimization_barrier((lows[0], full))
            if not last:
                us = [lax.all_gather(lows[0], "terms", axis=0, tiled=True)]
            if full is not None:
                krylov = write_vector(krylov, full, step_idx)
                if not last:
                    krylov, lows[1] = lax.optimization_barrier((krylov, lows[1]))
            if not last:
                *lows, late, us[0] = lax.optimization_barrier((*lows[1:], nxt, us[0]))
                us += [lax.all_gather(low, "terms", axis=0, tiled=True) for low in lows]
                full = lax.all_gather(late, "terms", axis=0, tiled=True)
            prev, cur = cur, nxt
            alphas.append(alpha[0, 0])
            betas.append(beta[0, 0])
        cut = 3 * pair * LANE
        head = lax.all_gather(late[:, :cut], "terms", axis=0, tiled=True)
        tail = lax.all_gather(late[:, cut:], "terms", axis=0, tiled=True)
        krylov = write_vector(krylov, head, LANCZOS_STEPS)
        krylov = write_vector(krylov, tail, LANCZOS_STEPS, cut // (pair * LANE))
        return krylov, jnp.stack(alphas), jnp.stack(betas)

    return jax.shard_map(body, mesh=mesh, in_specs=(P(), P("terms"), P("terms"), P("terms")), out_specs=(P(), P(), P()), check_vma=False)
```
